32 devices in a mesh: dp: 4 (over y, z), pp: 8 (over x, core).
Axes of the slice: x: 4, y: 2, z: 2, core: 2. Of those that a mesh axis runs over, the one named last changes fastest.
The devices are a block of a 4x4x8 slice.
Arguments:
- hidden: bfloat16 [32, 512, 960], P(('dp', 'pp')), parts along dimension 0
- labels: int32 [32, 512], P(('dp', 'pp')), parts along dimension 0
- gamma: float32 [960], replicated
- table: bfloat16 [49152, 960], P('pp')
Outputs:
- output 1: float32 [32, 512], P(('dp', 'pp')), parts along dimension 0
- output 2: bfloat16 [32, 512, 960], P(('dp', 'pp')), parts along dimension 0
- output 3: float32 [4], P('dp'), parts along dimension 0
- output 4: float32 [196608, 960], P(('dp', 'pp')), parts along dimension 0
- output 5: float32 [3840], P('dp'), parts along dimension 0
There are 4 independent parts. The reference program is written for one: setup_inputs(seed, part) draws one part's arguments, and reference() takes and returns one part's arrays. A program takes and returns all parts, laid end to end along the dimension named above; an argument that names none is the same for every part.
All inputs are finite; a program needn't handle non-finite values.
Results may differ from the reference program's by a relative error of at most 0.001.
Values are sent between devices in bfloat16 or wider.
A program may use at most 768 MiB of HBM per device.

```python
import jax
import jax.numpy as jnp
from jax import lax

MICROBATCHES = 8
SEQ_LEN = 512
D_MODEL = 960
VOCAB_SIZE = 49152
SOFT_CAP = 30
EPS = 1e-6
LOGIT_SCALE = 10.0


def setup_inputs(seed: int = 0, part: int = 0) -> dict:
    base_key = jax.random.key(seed)
    shared_key, part_base = jax.random.split(base_key)
    part_key = jax.random.fold_in(part_base, part)
    key_hidden, key_labels = jax.random.split(part_key)
    key_gain, key_table = jax.random.split(shared_key)
    hidden = jax.random.normal(key_hidden, (MICROBATCHES, SEQ_LEN, D_MODEL), jnp.float32).astype(jnp.bfloat16)
    labels = jax.random.randint(key_labels, (MICROBATCHES, SEQ_LEN), 0, VOCAB_SIZE, dtype=jnp.int32)
    gamma = 0.3 * jax.random.normal(key_gain, (D_MODEL,), jnp.float32)
    table_f = jax.random.normal(key_table, (VOCAB_SIZE, D_MODEL), jnp.float32) * (LOGIT_SCALE * D_MODEL ** -0.5)
    return {'hidden': hidden, 'labels': labels, 'gamma': gamma, 'table': table_f.astype(jnp.bfloat16)}


def norm_rows(rows, gain):
    mean_sq = jnp.mean(rows * rows, axis=-1, keepdims=True)
    return rows * lax.rsqrt(mean_sq + EPS) * (1.0 + gain)


def reference(hidden, labels, gamma, table):
    total = MICROBATCHES * SEQ_LEN
    vocab_ids = lax.broadcasted_iota(jnp.int32, (1, VOCAB_SIZE), 1)

    def micro_step(carry, scan_in):
        grad_table, grad_gain = carry
        block, block_labels = scan_in
        normed32, norm_vjp = jax.vjp(norm_rows, block.astype(jnp.float32), gamma)
        normed = normed32.astype(jnp.bfloat16)
        logits = jnp.dot(normed, table.T, preferred_element_type=jnp.float32)
        tanh_z = jnp.tanh(logits / SOFT_CAP)
        capped = SOFT_CAP * tanh_z
        row_max = jnp.max(capped, axis=1, keepdims=True)
        log_norm = row_max + jnp.log(jnp.sum(jnp.exp(capped - row_max), axis=1, keepdims=True))
        label_hit = vocab_ids == block_labels[:, None]
        label_logit = jnp.sum(jnp.where(label_hit, capped, 0.0), axis=1)
        tok_loss = log_norm[:, 0] - label_logit
        soft_probs = jnp.exp(capped - log_norm)
        grad_capped = jnp.where(label_hit, soft_probs - 1.0, soft_probs) / total
        grad_logits = (grad_capped * (1.0 - tanh_z * tanh_z)).astype(jnp.bfloat16)
        grad_normed = jnp.dot(grad_logits, table, preferred_element_type=jnp.float32)
        grad_block, gain_part = norm_vjp(grad_normed)
        table_part = jnp.dot(grad_logits.T, normed, preferred_element_type=jnp.float32)
        return (grad_table + table_part, grad_gain + gain_part), (tok_loss, grad_block.astype(jnp.bfloat16))

    init_acc = (jnp.zeros((VOCAB_SIZE, D_MODEL), jnp.float32), jnp.zeros((D_MODEL,), jnp.float32))
    (grad_table, grad_gain), (tok_loss, grad_hidden) = lax.scan(micro_step, init_acc, (hidden, labels))
    mean_loss = jnp.reshape(jnp.mean(tok_loss), (1,))
    return tok_loss, grad_hidden, mean_loss, grad_table, grad_gain
```

```python
import functools
import math

import jax
import jax.numpy as jnp
from jax import lax
from jax.experimental import pallas as pl
from jax.experimental.pallas import tpu as pltpu
from jax.sharding import PartitionSpec as P

SOFT_CAP = 30.0
EPS = 1e-6
CAP_LOG2E = SOFT_CAP * math.log2(math.e)
FWD_TILE = 1536
FWD_SUB = 512
BWD_TILE = 1024
BWD_SUB = 512
VMEM_LIMIT = 66_000_000


def norm_rows(rows, gain):
    mean_sq = jnp.mean(rows * rows, axis=-1, keepdims=True)
    return rows * lax.rsqrt(mean_sq + EPS) * (1.0 + gain)


def fold8(x):
    return jnp.sum(x.reshape(x.shape[0] // 8, 8, x.shape[1]), axis=0)


def fwd_kernel(n_tiles, labels_ref, normed_ref, w_hbm, t_ref, stats_ref, w_ref, w_sems):
    chunk, tile = pl.program_id(0), pl.program_id(1)

    def w_copy(i):
        rows = pl.ds(i * FWD_TILE, FWD_TILE)
        return pltpu.make_async_copy(w_hbm.at[rows, :], w_ref.at[rows, :], w_sems.at[i])

    @pl.when(chunk == 0)
    def _():
        @pl.when(tile == 0)
        def _():
            for i in range(n_tiles):
                w_copy(i).start()
        w_copy(tile).wait()

    @pl.when(tile == 0)
    def _():
        stats_ref[...] = jnp.zeros_like(stats_ref)

    row0 = pl.multiple_of(tile * FWD_TILE, FWD_TILE)
    normed = normed_ref[...]
    labels = labels_ref[...] - row0
    iota = lax.broadcasted_iota(jnp.int32, (FWD_SUB, normed.shape[0]), 0)
    exp_sum = stats_ref[0:8, :]
    label_sum = stats_ref[8:16, :]
    for s in range(FWD_TILE // FWD_SUB):
        w = w_ref[pl.ds(pl.multiple_of(row0 + s * FWD_SUB, FWD_SUB), FWD_SUB), :]
        z = lax.dot_general(w, normed, (((1,), (1,)), ((), ())), preferred_element_type=jnp.float32)
        t = jnp.tanh(z * (1.0 / SOFT_CAP))
        t_ref[s * FWD_SUB:(s + 1) * FWD_SUB, :] = t
        exp_sum += fold8(jnp.exp2(t * CAP_LOG2E))
        label_sum += fold8(jnp.where(iota == labels - s * FWD_SUB, t, 0.0))
    stats_ref[0:8, :] = exp_sum
    stats_ref[8:16, :] = label_sum


def forward(normed, labels, table):
    tokens, width = normed.shape
    vocab = table.shape[0]
    chunk = 512
    n_tiles = vocab // FWD_TILE
    return pl.pallas_call(
        functools.partial(fwd_kernel, n_tiles),
        grid=(tokens // chunk, n_tiles),
        in_specs=[
            pl.BlockSpec((1, chunk), lambda c, v: (0, c)),
            pl.BlockSpec((chunk, width), lambda c, v: (c, 0)),
            pl.BlockSpec(memory_space=pl.ANY),
        ],
        out_specs=[
            pl.BlockSpec((FWD_TILE, chunk), lambda c, v: (v, c)),
            pl.BlockSpec((16, chunk), lambda c, v: (0, c)),
        ],
        out_shape=[
            jax.ShapeDtypeStruct((vocab, tokens), jnp.float32),
            jax.ShapeDtypeStruct((16, tokens), jnp.float32),
        ],
        scratch_shapes=[pltpu.VMEM((vocab, width), table.dtype), pltpu.SemaphoreType.DMA((n_tiles,))],
        compiler_params=pltpu.CompilerParams(vmem_limit_bytes=VMEM_LIMIT),
        cost_estimate=pl.CostEstimate(flops=2 * tokens * vocab * width, transcendentals=2 * tokens * vocab,
                                      bytes_accessed=4 * tokens * vocab),
        name='head_fwd',
    )(labels, normed, table)


def bwd_kernel(n_chunks, n_tiles, total, labels_ref, inv_ref, normed_ref, t_ref, wt_ref, dn_ref, dw_hbm, dw_ref, dw_sems):
    chunk, tile = pl.program_id(0), pl.program_id(1)
    row0 = pl.multiple_of(tile * BWD_TILE, BWD_TILE)
    tile_rows = pl.ds(row0, BWD_TILE)

    @pl.when(tile == 0)
    def _():
        dn_ref[...] = jnp.zeros_like(dn_ref)

    @pl.when(chunk == 0)
    def _():
        dw_ref[tile_rows, :] = jnp.zeros((BWD_TILE, dw_ref.shape[1]), jnp.float32)

    normed = normed_ref[...]
    labels = labels_ref[...] - row0
    inv = inv_ref[...]
    iota = lax.broadcasted_iota(jnp.int32, (BWD_SUB, normed.shape[0]), 0)
    dz = []
    for s in range(BWD_TILE // BWD_SUB):
        t = t_ref[s * BWD_SUB:(s + 1) * BWD_SUB, :]
        p = jnp.exp2(t * CAP_LOG2E) * inv
        dc = jnp.where(iota == labels - s * BWD_SUB, p - 1.0 / total, p)
        dz.append((dc * (1.0 - t * t)).astype(jnp.bfloat16))
        rows = pl.ds(pl.multiple_of(row0 + s * BWD_SUB, BWD_SUB), BWD_SUB)
        dw_ref[rows, :] += jnp.dot(dz[-1], normed, preferred_element_type=jnp.float32)
    dz = jnp.concatenate(dz, axis=0)
    dn_ref[...] += jnp.dot(wt_ref[...], dz, preferred_element_type=jnp.float32)

    @pl.when(chunk == n_chunks - 1)
    def _():
        pltpu.make_async_copy(dw_ref.at[tile_rows, :], dw_hbm.at[tile_rows, :], dw_sems.at[tile]).start()

        @pl.when(tile == n_tiles - 1)
        def _():
            for i in range(n_tiles):
                rows = pl.ds(i * BWD_TILE, BWD_TILE)
                pltpu.make_async_copy(dw_ref.at[rows, :], dw_hbm.at[rows, :], dw_sems.at[i]).wait()


def backward(t, normed, labels, inv, table_t):
    vocab, tokens = t.shape
    width = normed.shape[1]
    chunk = 512
    n_chunks, n_tiles = tokens // chunk, vocab // BWD_TILE
    return pl.pallas_call(
        functools.partial(bwd_kernel, n_chunks, n_tiles, tokens),
        grid=(n_chunks, n_tiles),
        in_specs=[
            pl.BlockSpec((1, chunk), lambda c, v: (0, c)),
            pl.BlockSpec((1, chunk), lambda c, v: (0, c)),
            pl.BlockSpec((chunk, width), lambda c, v: (c, 0)),
            pl.BlockSpec((BWD_TILE, chunk), lambda c, v: (v, c)),
            pl.BlockSpec((width, BWD_TILE), lambda c, v: (0, v)),
        ],
        out_specs=[
            pl.BlockSpec((None, width, chunk), lambda c, v: (c, 0, 0)),
            pl.BlockSpec(memory_space=pl.ANY),
        ],
        out_shape=[
            jax.ShapeDtypeStruct((n_chunks, width, chunk), jnp.float32),
            jax.ShapeDtypeStruct((vocab, width), jnp.float32),
        ],
        scratch_shapes=[pltpu.VMEM((vocab, width), jnp.float32), pltpu.SemaphoreType.DMA((n_tiles,))],
        compiler_params=pltpu.CompilerParams(vmem_limit_bytes=VMEM_LIMIT),
        cost_estimate=pl.CostEstimate(flops=4 * tokens * vocab * width, transcendentals=tokens * vocab,
                                      bytes_accessed=4 * tokens * vocab),
        name='head_bwd',
    )(labels, inv, normed, t, table_t)


def solution(mesh):
    def local_fn(hidden, labels, gamma, table):
        mb_dev, seq_len, width = hidden.shape
        v_shard = table.shape[0]
        rank = lax.axis_index('pp')
        own = mb_dev * seq_len
        normed32, norm_vjp = jax.vjp(norm_rows, hidden.astype(jnp.float32).reshape(own, width), gamma)
        normed = lax.all_gather(normed32.astype(jnp.bfloat16), 'pp', axis=0, tiled=True)
        all_labels = lax.all_gather(labels.reshape(1, own), 'pp', axis=1, tiled=True)
        total = normed.shape[0]
        local_labels = all_labels - rank * v_shard
        t, stats = forward(normed, local_labels, table)
        stats = lax.psum(jnp.sum(stats.reshape(2, 8, total), axis=1), 'pp')
        all_loss = jnp.log(stats[0]) - SOFT_CAP * stats[1]
        inv = (1.0 / (stats[0] * total))[None, :]
        dn, grad_table = backward(t, normed, local_labels, inv, table.T)
        own_dn = lax.psum_scatter(dn, 'pp', scatter_dimension=0, tiled=True)[0].T
        grad_rows, grad_gain = norm_vjp(own_dn)
        grad_gain = lax.psum(grad_gain, 'pp')
        own_loss = lax.dynamic_slice_in_dim(all_loss, rank * own, own, axis=0).reshape(mb_dev, seq_len)
        mean_loss = jnp.reshape(jnp.mean(all_loss), (1,))
        grad_hidden = grad_rows.astype(jnp.bfloat16).reshape(mb_dev, seq_len, width)
        return own_loss, grad_hidden, mean_loss, grad_table, grad_gain

    token_spec = P(('dp', 'pp'))
    return jax.shard_map(local_fn, mesh=mesh,
                         in_specs=(token_spec, token_spec, P(), P('pp')),
                         out_specs=(token_spec, token_spec, P('dp'), token_spec, P('dp')),
                         check_vma=False)
```

```python
import functools
import math

import jax
import jax.numpy as jnp
from jax import lax
from jax.experimental import pallas as pl
from jax.experimental.pallas import tpu as pltpu
from jax.sharding import PartitionSpec as P

SOFT_CAP = 30.0
EPS = 1e-6
CAP_LOG2E = SOFT_CAP * math.log2(math.e)
FWD_TILE = 1536
BWD_TILE = 1024
SUB = 512
LANES = 128
VMEM_LIMIT = 66_000_000
AXIS = 'pp'
MESH_ID = pl.DeviceIdType.MESH
ANY = pl.BlockSpec(memory_space=pl.ANY)


def norm_cols(cols, gain):
    mean_sq = jnp.mean(cols * cols, axis=0, keepdims=True)
    return cols * lax.rsqrt(mean_sq + EPS) * (1.0 + gain[:, None])


def fold_lanes(x):
    return sum(x[:, i:i + LANES] for i in range(0, x.shape[1], LANES))


def spread(col, width):
    return jnp.concatenate([col] * (width // LANES), axis=1)


def row_to_col(row):
    return jnp.broadcast_to(row, (LANES, row.shape[1])).T


def enter(n):
    me = lax.axis_index(AXIS)
    barrier = pltpu.get_barrier_semaphore()
    for d in range(1, n):
        pl.semaphore_signal(barrier, inc=1, device_id={AXIS: lax.rem(me + d, n)}, device_id_type=MESH_ID)


def entered(n):
    pl.semaphore_wait(pltpu.get_barrier_semaphore(), n - 1)


def remote(src, dst, send_sem, recv_sem, peer):
    return pltpu.make_async_remote_copy(src_ref=src, dst_ref=dst, send_sem=send_sem, recv_sem=recv_sem,
                                        device_id={AXIS: peer}, device_id_type=MESH_ID)


def fwd_offset(step, n):
    half = (step + 1) // 2
    return lax.rem(jnp.where(lax.rem(step, 2) == 1, n - half, half), n)


def fwd_kernel(n, n_tiles, labels_hbm, own_hbm, w_hbm, tr_ref, tl_ref, n_hbm, labels_out, stats_out,
               w_ref, cols_ref, labels_ref, stats_ref, rows_ref, label_ref, exp_ref, hit_ref,
               w_sems, in_sems, out_sems, right_send, right_recv, left_send, left_recv,
               lab_send, lab_recv, stat_send, stat_recv):
    step, tile = pl.program_id(0), pl.program_id(1)
    me = lax.axis_index(AXIS)
    right, left = lax.rem(me + 1, n), lax.rem(me + n - 1, n)
    vocab = w_ref.shape[1]
    half = rows_ref.shape[0] // 2
    last = n - 1
    offset = fwd_offset(step, n)
    chunk = lax.rem(me + offset, n)

    def w_copy(i):
        cols = pl.ds(pl.multiple_of(i * FWD_TILE, FWD_TILE), FWD_TILE)
        return pltpu.make_async_copy(w_hbm.at[:, cols], w_ref.at[:, cols], w_sems.at[i])

    def hop(j, to_right):
        if to_right:
            src, dst, sends, recvs, peer = max(2 * j - 3, 0), 2 * j - 1, right_send, right_recv, right
        else:
            src, dst, sends, recvs, peer = 2 * j - 2, 2 * j, left_send, left_recv, left
        return remote(cols_ref.at[src], cols_ref.at[dst], sends.at[j], recvs.at[j], peer)

    def label_copy(d):
        return remote(labels_ref.at[me], labels_ref.at[me], lab_send.at[d], lab_recv.at[d], lax.rem(me + d, n))

    def label_arrival(d):
        src = lax.rem(me + n - d, n)
        return remote(labels_ref.at[src], labels_ref.at[src], lab_send.at[d], lab_recv.at[d], src)

    def stat_copy(k, d):
        slot = lax.rem(me + fwd_offset(k, n), n)
        return remote(stats_ref.at[me, slot], stats_ref.at[me, slot], stat_send.at[k, d], stat_recv.at[k, d],
                      lax.rem(me + d, n))

    def stat_arrival(k, d):
        src = lax.rem(me + n - d, n)
        slot = lax.rem(src + fwd_offset(k, n), n)
        return remote(stats_ref.at[src, slot], stats_ref.at[src, slot], stat_send.at[k, d], stat_recv.at[k, d], src)

    def n_copies(k):
        off = fwd_offset(k, n)
        to_r, to_l = lax.rem(2 * n - 1 - off, n), lax.rem(off + n - 1, n)
        return [pltpu.make_async_copy(cols_ref.at[k, :, 0:half], n_hbm.at[to_r, :, 0:half], out_sems.at[0, k]),
                pltpu.make_async_copy(cols_ref.at[k, :, half:2 * half], n_hbm.at[to_l, :, half:2 * half],
                                      out_sems.at[1, k])]

    right_hops, left_hops = n // 2, (n - 1) // 2

    @pl.when((step == 0) & (tile == 0))
    def _():
        enter(n)
        own = [pltpu.make_async_copy(own_hbm, cols_ref.at[0], in_sems.at[0]),
               pltpu.make_async_copy(labels_hbm, labels_ref.at[me], in_sems.at[1])]
        for copy in own:
            copy.start()
        for i in range(n_tiles):
            w_copy(i).start()
        for copy in own:
            copy.wait()
        entered(n)
        hop(1, True).start()
        hop(1, False).start()
        for d in range(1, n):
            label_copy(d).start()

    for j in range(1, right_hops + 1):
        @pl.when((step == 2 * j - 1) & (tile == 0))
        def _(j=j):
            hop(j, True).wait_recv()
            if j < right_hops:
                hop(j + 1, True).start()
            if j <= left_hops:
                hop(j, False).wait_recv()
            if j < left_hops:
                hop(j + 1, False).start()
            if j == 1:
                for d in range(1, n):
                    label_arrival(d).wait_recv()

    @pl.when((step > 0) & (tile == 0))
    def _():
        for d in range(1, n):
            stat_copy(step - 1, d).start()

    @pl.when(step == 0)
    def _():
        w_copy(tile).wait()

    @pl.when(tile == 0)
    def _():
        for copy in n_copies(step):
            copy.start()
        rows_ref[...] = cols_ref[step].T
        label_ref[...] = row_to_col(labels_ref[chunk]) - me * vocab
        exp_ref[...] = jnp.zeros_like(exp_ref)
        hit_ref[...] = jnp.zeros_like(hit_ref)

    rows = rows_ref[...]
    col0 = pl.multiple_of(tile * FWD_TILE, FWD_TILE)
    labels = label_ref[...] - col0
    iota = lax.broadcasted_iota(jnp.int32, (rows.shape[0], SUB), 1)
    exp_sum = exp_ref[...]
    label_sum = hit_ref[...]
    for s in range(FWD_TILE // SUB):
        w = w_ref[:, pl.ds(pl.multiple_of(col0 + s * SUB, SUB), SUB)]
        z = jnp.dot(rows, w, preferred_element_type=jnp.float32)
        t = jnp.tanh(z * (1.0 / SOFT_CAP))
        tr_ref[:, s * SUB:(s + 1) * SUB] = t[0:half]
        tl_ref[:, s * SUB:(s + 1) * SUB] = t[half:2 * half]
        exp_sum += fold_lanes(jnp.exp2(t * CAP_LOG2E))
        label_sum += fold_lanes(jnp.where(iota == spread(labels - s * SUB, SUB), t, 0.0))
    exp_ref[...] = exp_sum
    hit_ref[...] = label_sum

    @pl.when(tile == n_tiles - 1)
    def _():
        stats_ref[me, chunk, 0:1, :] = jnp.sum(exp_ref[...].T, axis=0, keepdims=True)
        stats_ref[me, chunk, 1:2, :] = jnp.sum(hit_ref[...].T, axis=0, keepdims=True)

    @pl.when((step == last) & (tile == n_tiles - 1))
    def _():
        labels_copy = pltpu.make_async_copy(labels_ref, labels_out, in_sems.at[1])
        labels_copy.start()
        for k in range(last):
            for d in range(1, n):
                stat_arrival(k, d).wait_recv()
                stat_copy(k, d).wait_send()
        for d in range(1, n):
            stat_copy(last, d).start()
        for j in range(1, right_hops + 1):
            hop(j, True).wait_send()
        for j in range(1, left_hops + 1):
            hop(j, False).wait_send()
        for d in range(1, n):
            label_copy(d).wait_send()
        for k in range(n):
            for copy in n_copies(k):
                copy.wait()
        labels_copy.wait()
        for d in range(1, n):
            stat_arrival(last, d).wait_recv()
        stats_out[...] = sum(stats_ref[i] for i in range(n))
        for d in range(1, n):
            stat_copy(last, d).wait_send()


def forward(n, normed, labels, table_t):
    width, chunk = normed.shape
    vocab = table_t.shape[1]
    tokens, half = n * chunk, chunk // 2
    n_tiles = vocab // FWD_TILE
    dma = pltpu.SemaphoreType.DMA

    def to_r(k, v):
        return lax.rem(2 * n - 1 - fwd_offset(k, n), n), 0, v

    def to_l(k, v):
        return lax.rem(fwd_offset(k, n) + n - 1, n), 0, v

    return pl.pallas_call(
        functools.partial(fwd_kernel, n, n_tiles),
        grid=(n, n_tiles),
        in_specs=[ANY, ANY, ANY],
        out_specs=[
            pl.BlockSpec((None, half, FWD_TILE), to_r),
            pl.BlockSpec((None, half, FWD_TILE), to_l),
            ANY,
            ANY,
            pl.BlockSpec((n, 2, chunk), lambda k, v: (0, 0, 0)),
        ],
        out_shape=[
            jax.ShapeDtypeStruct((n, half, vocab), jnp.float32),
            jax.ShapeDtypeStruct((n, half, vocab), jnp.float32),
            jax.ShapeDtypeStruct((n, width, chunk), normed.dtype),
            jax.ShapeDtypeStruct((n, 1, chunk), jnp.int32),
            jax.ShapeDtypeStruct((n, 2, chunk), jnp.float32),
        ],
        scratch_shapes=[
            pltpu.VMEM((width, vocab), table_t.dtype),
            pltpu.VMEM((n, width, chunk), normed.dtype),
            pltpu.VMEM((n, 1, chunk), jnp.int32),
            pltpu.VMEM((n, n, 2, chunk), jnp.float32),
            pltpu.VMEM((chunk, width), normed.dtype),
            pltpu.VMEM((chunk, LANES), jnp.int32),
            pltpu.VMEM((chunk, LANES), jnp.float32),
            pltpu.VMEM((chunk, LANES), jnp.float32),
            dma((n_tiles,)), dma((2,)), dma((2, n)), dma((n,)), dma((n,)), dma((n,)), dma((n,)),
            dma((n,)), dma((n,)), dma((n, n)), dma((n, n)),
        ],
        compiler_params=pltpu.CompilerParams(vmem_limit_bytes=VMEM_LIMIT, collective_id=0, has_side_effects=True),
        cost_estimate=pl.CostEstimate(flops=2 * tokens * vocab * width, transcendentals=2 * tokens * vocab,
                                      bytes_accessed=4 * tokens * vocab),
        name='head_fwd',
    )(labels, normed, table_t)


def bwd_kernel(n, n_tiles, total, labels_hbm, stats_hbm, hidden_hbm, gain_hbm, normed_ref, tr_ref, tl_ref, w_ref,
               dw_hbm, dh_hbm, dgain_ref,
               dw_ref, dn_ref, ring_ref, label_ref, scale_ref, labels_ref, stats_ref, hidden_ref, gain_ref, dh_ref, gains_ref,
               dw_sems, in_sems, ring_send, ring_recv, gain_send, gain_recv):
    step, tile = pl.program_id(0), pl.program_id(1)
    me = lax.axis_index(AXIS)
    right, left = lax.rem(me + 1, n), lax.rem(me + n - 1, n)
    vocab = dw_ref.shape[1]
    half = tr_ref.shape[0]
    last = n - 1
    from_r, from_l = lax.rem(me + 2 * n - 1 - step, n), lax.rem(me + 1 + step, n)
    col0 = pl.multiple_of(tile * BWD_TILE, BWD_TILE)
    tile_cols = pl.ds(col0, BWD_TILE)

    def pass_on(k, way):
        return remote(ring_ref.at[k, way], ring_ref.at[k + 1, way], ring_send.at[way, k], ring_recv.at[way, k],
                      (right, left)[way])

    def gain_copy(d):
        return remote(gains_ref.at[me], gains_ref.at[me], gain_send.at[d], gain_recv.at[d], lax.rem(me + d, n))

    def gain_arrival(d):
        src = lax.rem(me + n - d, n)
        return remote(gains_ref.at[src], gains_ref.at[src], gain_send.at[d], gain_recv.at[d], src)

    loads = [pltpu.make_async_copy(src, dst, in_sems.at[i]) for i, (src, dst) in enumerate(
        [(labels_hbm, labels_ref), (stats_hbm, stats_ref), (hidden_hbm, hidden_ref), (gain_hbm, gain_ref)])]

    @pl.when((step == 0) & (tile == 0))
    def _():
        enter(n)
        for copy in loads:
            copy.start()
        for copy in loads:
            copy.wait()
        entered(n)

    @pl.when((step > 0) & (tile == 0))
    def _():
        for way in range(2):
            pass_on(step - 1, way).start()

    @pl.when(tile == 0)
    def _():
        dn_ref[...] = jnp.zeros_like(dn_ref)
        labels = jnp.concatenate([labels_ref[from_r][:, 0:half], labels_ref[from_l][:, half:2 * half]], axis=1)
        label_ref[...] = row_to_col(labels) - me * vocab
        sums = jnp.concatenate([stats_ref[from_r, 0:1, 0:half], stats_ref[from_l, 0:1, half:2 * half]], axis=1)
        scale_ref[...] = row_to_col(1.0 / (sums * total))

    @pl.when(step == 0)
    def _():
        dw_ref[:, tile_cols] = jnp.zeros((dw_ref.shape[0], BWD_TILE), jnp.float32)

    normed = normed_ref[...]
    labels = label_ref[...] - col0
    scale = spread(scale_ref[...], SUB)
    iota = lax.broadcasted_iota(jnp.int32, (half, SUB), 1)
    dz = []
    for s in range(BWD_TILE // SUB):
        parts = []
        for h, t_ref in enumerate((tr_ref, tl_ref)):
            rows = slice(h * half, (h + 1) * half)
            t = t_ref[:, s * SUB:(s + 1) * SUB]
            p = jnp.exp2(t * CAP_LOG2E) * scale[rows]
            dc = jnp.where(iota == spread(labels[rows] - s * SUB, SUB), p - 1.0 / total, p)
            parts.append((dc * (1.0 - t * t)).astype(jnp.bfloat16))
        dz.append(jnp.concatenate(parts, axis=0))
        cols = pl.ds(pl.multiple_of(col0 + s * SUB, SUB), SUB)
        dw_ref[:, cols] += jnp.dot(normed, dz[-1], preferred_element_type=jnp.float32)
    dz = jnp.concatenate(dz, axis=1)
    dn_ref[...] += lax.dot_general(w_ref[...], dz, (((1,), (1,)), ((), ())), preferred_element_type=jnp.float32)

    @pl.when(step == last)
    def _():
        pltpu.make_async_copy(dw_ref.at[:, tile_cols], dw_hbm.at[:, tile_cols], dw_sems.at[tile]).start()

    @pl.when((step == 0) & (tile == n_tiles - 1))
    def _():
        ring_ref[0, 0] = dn_ref[:, 0:half]
        ring_ref[0, 1] = dn_ref[:, half:2 * half]

    @pl.when((step > 0) & (tile == n_tiles - 1))
    def _():
        for way in range(2):
            pass_on(step - 1, way).wait_recv()
            ring_ref[step, way] += dn_ref[:, way * half:(way + 1) * half]

    @pl.when((step == last) & (tile == n_tiles - 1))
    def _():
        width = hidden_ref.shape[0]
        gain = 1.0 + gain_ref[...]
        folds = []
        for way in range(2):
            cols = slice(way * half, (way + 1) * half)
            x = hidden_ref[:, cols].astype(jnp.float32)
            dn = ring_ref[last, way]
            r = lax.rsqrt(jnp.mean(x * x, axis=0, keepdims=True) + EPS)
            folds.append(fold_lanes(dn * x * r))
            dy = dn * gain
            dot = jnp.sum(dy * x, axis=0, keepdims=True)
            dh_ref[:, cols] = (dy * r - x * (r * r * r * dot * (1.0 / width))).astype(dh_ref.dtype)
        gains_ref[me] = jnp.sum((folds[0] + folds[1]).T, axis=0, keepdims=True)
        dh_copy = pltpu.make_async_copy(dh_ref, dh_hbm, in_sems.at[0])
        dh_copy.start()
        for k in range(last):
            for way in range(2):
                pass_on(k, way).wait_send()
        for d in range(1, n):
            gain_copy(d).start()
        for i in range(n_tiles):
            cols = pl.ds(i * BWD_TILE, BWD_TILE)
            pltpu.make_async_copy(dw_ref.at[:, cols], dw_hbm.at[:, cols], dw_sems.at[i]).wait()
        dh_copy.wait()
        for d in range(1, n):
            gain_arrival(d).wait_recv()
        dgain_ref[...] = sum(gains_ref[i] for i in range(n))
        for d in range(1, n):
            gain_copy(d).wait_send()


def backward(n, labels, stats, hidden_t, gain, normed, t_r, t_l, table_t):
    _, width, chunk = normed.shape
    vocab = table_t.shape[1]
    tokens, half = n * chunk, chunk // 2
    n_tiles = vocab // BWD_TILE
    dma = pltpu.SemaphoreType.DMA
    return pl.pallas_call(
        functools.partial(bwd_kernel, n, n_tiles, tokens),
        grid=(n, n_tiles),
        in_specs=[
            ANY, ANY, ANY, ANY,
            pl.BlockSpec((None, width, chunk), lambda s, v: (s, 0, 0)),
            pl.BlockSpec((None, half, BWD_TILE), lambda s, v: (s, 0, v)),
            pl.BlockSpec((None, half, BWD_TILE), lambda s, v: (s, 0, v)),
            pl.BlockSpec((width, BWD_TILE), lambda s, v: (0, v)),
        ],
        out_specs=[ANY, ANY, pl.BlockSpec((1, width), lambda s, v: (0, 0))],
        out_shape=[
            jax.ShapeDtypeStruct((width, vocab), jnp.float32),
            jax.ShapeDtypeStruct((width, chunk), jnp.bfloat16),
            jax.ShapeDtypeStruct((1, width), jnp.float32),
        ],
        scratch_shapes=[
            pltpu.VMEM((width, vocab), jnp.float32),
            pltpu.VMEM((width, chunk), jnp.float32),
            pltpu.VMEM((n, 2, width, half), jnp.float32),
            pltpu.VMEM((chunk, LANES), jnp.int32),
            pltpu.VMEM((chunk, LANES), jnp.float32),
            pltpu.VMEM((n, 1, chunk), jnp.int32),
            pltpu.VMEM((n, 2, chunk), jnp.float32),
            pltpu.VMEM((width, chunk), jnp.bfloat16),
            pltpu.VMEM((width, 1), jnp.float32),
            pltpu.VMEM((width, chunk), jnp.bfloat16),
            pltpu.VMEM((n, 1, width), jnp.float32),
            dma((n_tiles,)), dma((4,)), dma((2, n)), dma((2, n)), dma((n,)), dma((n,)),
        ],
        compiler_params=pltpu.CompilerParams(vmem_limit_bytes=VMEM_LIMIT, collective_id=1, has_side_effects=True),
        cost_estimate=pl.CostEstimate(flops=4 * tokens * vocab * width, transcendentals=tokens * vocab,
                                      bytes_accessed=4 * tokens * vocab),
        name='head_bwd',
    )(labels, stats, hidden_t, gain, normed, t_r, t_l, table_t)


def solution(mesh):
    n = mesh.shape[AXIS]

    def local_fn(hidden, labels, gamma, table):
        mb_dev, seq_len, width = hidden.shape
        rank = lax.axis_index(AXIS)
        own = mb_dev * seq_len
        hidden_t = hidden.reshape(own, width).T
        normed = norm_cols(hidden_t.astype(jnp.float32), gamma).astype(jnp.bfloat16)
        table_t = table.T
        t_r, t_l, all_normed, all_labels, stats = forward(n, normed, labels.reshape(1, own), table_t)
        all_loss = jnp.log(stats[:, 0]) - SOFT_CAP * stats[:, 1]
        grad_table_t, grad_hidden_t, grad_gain = backward(n, all_labels, stats, hidden_t, gamma[:, None], all_normed,
                                                          t_r, t_l, table_t)
        own_loss = lax.dynamic_slice_in_dim(all_loss, rank, 1, axis=0).reshape(mb_dev, seq_len)
        mean_loss = jnp.reshape(jnp.mean(all_loss), (1,))
        grad_hidden = grad_hidden_t.T.reshape(mb_dev, seq_len, width)
        return own_loss, grad_hidden, mean_loss, grad_table_t.T, grad_gain[0]

    token_spec = P(('dp', 'pp'))
    return jax.shard_map(local_fn, mesh=mesh,
                         in_specs=(token_spec, token_spec, P(), P('pp')),
                         out_specs=(token_spec, token_spec, P('dp'), token_spec, P('dp')),
                         check_vma=False)
```

```python
import functools
import math

import jax
import jax.numpy as jnp
from jax import lax
from jax.experimental import pallas as pl
from jax.experimental.pallas import tpu as pltpu
from jax.sharding import PartitionSpec as P

SOFT_CAP = 30.0
EPS = 1e-6
CAP_LOG2E = SOFT_CAP * math.log2(math.e)
FWD_TILE = 3072
BWD_TILE = 2048
LATE_TILES = 1
SUB = 512
LANES = 128
VMEM_LIMIT = 66_000_000
AXIS = 'pp'
MESH_ID = pl.DeviceIdType.MESH
ANY = pl.BlockSpec(memory_space=pl.ANY)


def fold_lanes(x):
    return sum(x[:, i:i + LANES] for i in range(0, x.shape[1], LANES))


def spread(col, width):
    return jnp.concatenate([col] * (width // LANES), axis=1)


def row_to_col(row):
    return jnp.broadcast_to(row, (LANES, row.shape[1])).T


def enter(n):
    me = lax.axis_index(AXIS)
    barrier = pltpu.get_barrier_semaphore()
    for d in range(1, n):
        pl.semaphore_signal(barrier, inc=1, device_id={AXIS: lax.rem(me + d, n)}, device_id_type=MESH_ID)


def entered(n):
    pl.semaphore_wait(pltpu.get_barrier_semaphore(), n - 1)


def remote(src, dst, send_sem, recv_sem, peer):
    return pltpu.make_async_remote_copy(src_ref=src, dst_ref=dst, send_sem=send_sem, recv_sem=recv_sem,
                                        device_id={AXIS: peer}, device_id_type=MESH_ID)


def fwd_offset(step, n):
    half = (step + 1) // 2
    return lax.rem(jnp.where(lax.rem(step, 2) == 1, n - half, half), n)


def fwd_kernel(n, n_tiles, labels_hbm, hidden_hbm, gain_hbm, w_hbm, tr_ref, tl_ref, n_hbm, labels_out, stats_out,
               w_ref, cols_ref, labels_ref, stats_ref, rows_ref, label_ref, exp_ref, hit_ref, hidden_ref, gain_ref,
               w_sems, in_sems, out_sems, right_send, right_recv, left_send, left_recv,
               lab_send, lab_recv, stat_send, stat_recv):
    step, tile = pl.program_id(0), pl.program_id(1)
    me = lax.axis_index(AXIS)
    right, left = lax.rem(me + 1, n), lax.rem(me + n - 1, n)
    vocab = w_ref.shape[1]
    half = rows_ref.shape[0] // 2
    last = n - 1
    offset = fwd_offset(step, n)
    chunk = lax.rem(me + offset, n)

    def w_copy(i):
        cols = pl.ds(pl.multiple_of(i * FWD_TILE, FWD_TILE), FWD_TILE)
        return pltpu.make_async_copy(w_hbm.at[:, cols], w_ref.at[:, cols], w_sems.at[i])

    def hop(j, to_right):
        if to_right:
            src, dst, sends, recvs, peer = max(2 * j - 3, 0), 2 * j - 1, right_send, right_recv, right
        else:
            src, dst, sends, recvs, peer = 2 * j - 2, 2 * j, left_send, left_recv, left
        return remote(cols_ref.at[src], cols_ref.at[dst], sends.at[j], recvs.at[j], peer)

    def label_copy(d):
        return remote(labels_ref.at[me], labels_ref.at[me], lab_send.at[d], lab_recv.at[d], lax.rem(me + d, n))

    def label_arrival(d):
        src = lax.rem(me + n - d, n)
        return remote(labels_ref.at[src], labels_ref.at[src], lab_send.at[d], lab_recv.at[d], src)

    def stat_copy(k, d):
        slot = lax.rem(me + fwd_offset(k, n), n)
        return remote(stats_ref.at[me, slot], stats_ref.at[me, slot], stat_send.at[k, d], stat_recv.at[k, d],
                      lax.rem(me + d, n))

    def stat_arrival(k, d):
        src = lax.rem(me + n - d, n)
        slot = lax.rem(src + fwd_offset(k, n), n)
        return remote(stats_ref.at[src, slot], stats_ref.at[src, slot], stat_send.at[k, d], stat_recv.at[k, d], src)

    def n_copies(k):
        off = fwd_offset(k, n)
        to_r, to_l = lax.rem(2 * n - 1 - off, n), lax.rem(off + n - 1, n)
        return [pltpu.make_async_copy(cols_ref.at[k, :, 0:half], n_hbm.at[to_r, :, 0:half], out_sems.at[0, k]),
                pltpu.make_async_copy(cols_ref.at[k, :, half:2 * half], n_hbm.at[to_l, :, half:2 * half],
                                      out_sems.at[1, k])]

    right_hops, left_hops = n // 2, (n - 1) // 2

    @pl.when((step == 0) & (tile == 0))
    def _():
        enter(n)
        own = [pltpu.make_async_copy(hidden_hbm, hidden_ref, in_sems.at[0]),
               pltpu.make_async_copy(labels_hbm, labels_ref.at[me], in_sems.at[1]),
               pltpu.make_async_copy(gain_hbm, gain_ref, in_sems.at[2])]
        for copy in own:
            copy.start()
        for i in range(n_tiles):
            w_copy(i).start()
        for copy in own:
            copy.wait()
        x = hidden_ref[...].astype(jnp.float32)
        scale = lax.rsqrt(jnp.mean(x * x, axis=0, keepdims=True) + EPS)
        cols_ref[0] = (x * scale * (1.0 + gain_ref[...])).astype(cols_ref.dtype)
        entered(n)
        hop(1, True).start()
        hop(1, False).start()
        for d in range(1, n):
            label_copy(d).start()

    for j in range(1, right_hops + 1):
        @pl.when((step == 2 * j - 1) & (tile == 0))
        def _(j=j):
            hop(j, True).wait_recv()
            if j < right_hops:
                hop(j + 1, True).start()
            if j <= left_hops:
                hop(j, False).wait_recv()
            if j < left_hops:
                hop(j + 1, False).start()
            if j == 1:
                for d in range(1, n):
                    label_arrival(d).wait_recv()

    @pl.when((step > 0) & (tile == 0))
    def _():
        for d in range(1, n):
            stat_copy(step - 1, d).start()

    @pl.when(step == 0)
    def _():
        w_copy(tile).wait()

    @pl.when(tile == 0)
    def _():
        for copy in n_copies(step):
            copy.start()
        rows_ref[...] = cols_ref[step].T
        label_ref[...] = row_to_col(labels_ref[chunk]) - me * vocab
        exp_ref[...] = jnp.zeros_like(exp_ref)
        hit_ref[...] = jnp.zeros_like(hit_ref)

    rows = rows_ref[...]
    col0 = pl.multiple_of(tile * FWD_TILE, FWD_TILE)
    labels = label_ref[...] - col0
    iota = lax.broadcasted_iota(jnp.int32, (rows.shape[0], SUB), 1)
    for s in range(FWD_TILE // SUB):
        w = w_ref[:, pl.ds(pl.multiple_of(col0 + s * SUB, SUB), SUB)]
        for r in range(0, 2 * half, LANES):
            row = slice(r, r + LANES)
            z = jnp.dot(rows[row], w, preferred_element_type=jnp.float32)
            t = jnp.tanh(z * (1.0 / SOFT_CAP))
            out = tr_ref if r < half else tl_ref
            out[r % half:r % half + LANES, s * SUB:(s + 1) * SUB] = t
            exp_ref[row, :] += fold_lanes(jnp.exp2(t * CAP_LOG2E))
            hit_ref[row, :] += fold_lanes(jnp.where(iota[row] == spread(labels[row] - s * SUB, SUB), t, 0.0))

    @pl.when(tile == n_tiles - 1)
    def _():
        stats_ref[me, chunk, 0:1, :] = jnp.sum(exp_ref[...].T, axis=0, keepdims=True)
        stats_ref[me, chunk, 1:2, :] = jnp.sum(hit_ref[...].T, axis=0, keepdims=True)

    @pl.when((step == last) & (tile == n_tiles - 1))
    def _():
        labels_copy = pltpu.make_async_copy(labels_ref, labels_out, in_sems.at[1])
        labels_copy.start()
        for k in range(last):
            for d in range(1, n):
                stat_arrival(k, d).wait_recv()
                stat_copy(k, d).wait_send()
        for d in range(1, n):
            stat_copy(last, d).start()
        for j in range(1, right_hops + 1):
            hop(j, True).wait_send()
        for j in range(1, left_hops + 1):
            hop(j, False).wait_send()
        for d in range(1, n):
            label_copy(d).wait_send()
        for k in range(n):
            for copy in n_copies(k):
                copy.wait()
        labels_copy.wait()
        for d in range(1, n):
            stat_arrival(last, d).wait_recv()
        stats_out[...] = sum(stats_ref[i] for i in range(n))
        for d in range(1, n):
            stat_copy(last, d).wait_send()


def forward(n, hidden_t, gain, labels, table_t):
    width, chunk = hidden_t.shape
    vocab = table_t.shape[1]
    tokens, half = n * chunk, chunk // 2
    n_tiles = vocab // FWD_TILE
    dma = pltpu.SemaphoreType.DMA

    def to_r(k, v):
        return lax.rem(2 * n - 1 - fwd_offset(k, n), n), 0, v

    def to_l(k, v):
        return lax.rem(fwd_offset(k, n) + n - 1, n), 0, v

    return pl.pallas_call(
        functools.partial(fwd_kernel, n, n_tiles),
        grid=(n, n_tiles),
        in_specs=[ANY, ANY, ANY, ANY],
        out_specs=[
            pl.BlockSpec((None, half, FWD_TILE), to_r),
            pl.BlockSpec((None, half, FWD_TILE), to_l),
            ANY,
            ANY,
            pl.BlockSpec((n, 2, chunk), lambda k, v: (0, 0, 0)),
        ],
        out_shape=[
            jax.ShapeDtypeStruct((n, half, vocab), jnp.float32),
            jax.ShapeDtypeStruct((n, half, vocab), jnp.float32),
            jax.ShapeDtypeStruct((n, width, chunk), jnp.bfloat16),
            jax.ShapeDtypeStruct((n, 1, chunk), jnp.int32),
            jax.ShapeDtypeStruct((n, 2, chunk), jnp.float32),
        ],
        scratch_shapes=[
            pltpu.VMEM((width, vocab), table_t.dtype),
            pltpu.VMEM((n, width, chunk), jnp.bfloat16),
            pltpu.VMEM((n, 1, chunk), jnp.int32),
            pltpu.VMEM((n, n, 2, chunk), jnp.float32),
            pltpu.VMEM((chunk, width), jnp.bfloat16),
            pltpu.VMEM((chunk, LANES), jnp.int32),
            pltpu.VMEM((chunk, LANES), jnp.float32),
            pltpu.VMEM((chunk, LANES), jnp.float32),
            pltpu.VMEM((width, chunk), hidden_t.dtype),
            pltpu.VMEM((width, 1), jnp.float32),
            dma((n_tiles,)), dma((3,)), dma((2, n)), dma((n,)), dma((n,)), dma((n,)), dma((n,)),
            dma((n,)), dma((n,)), dma((n, n)), dma((n, n)),
        ],
        compiler_params=pltpu.CompilerParams(vmem_limit_bytes=VMEM_LIMIT, collective_id=0, has_side_effects=True),
        cost_estimate=pl.CostEstimate(flops=2 * tokens * vocab * width, transcendentals=2 * tokens * vocab,
                                      bytes_accessed=4 * tokens * vocab),
        name='head_fwd',
    )(labels, hidden_t, gain, table_t)


def bwd_kernel(n, n_tiles, total, labels_hbm, stats_hbm, hidden_hbm, gain_hbm, normed_ref, tr_ref, tl_ref, w_ref,
               dw_hbm, dz_ref, dh_hbm, dgain_ref,
               dw_ref, dn_ref, ring_ref, label_ref, scale_ref, labels_ref, stats_ref, hidden_ref, gain_ref, dh_ref, gains_ref,
               dw_sems, in_sems, ring_send, ring_recv, gain_send, gain_recv):
    step, tile = pl.program_id(0), pl.program_id(1)
    me = lax.axis_index(AXIS)
    right, left = lax.rem(me + 1, n), lax.rem(me + n - 1, n)
    vocab = n_tiles * BWD_TILE
    n_early = n_tiles - LATE_TILES
    half = tr_ref.shape[0]
    last = n - 1
    from_r, from_l = lax.rem(me + 2 * n - 1 - step, n), lax.rem(me + 1 + step, n)
    col0 = pl.multiple_of(tile * BWD_TILE, BWD_TILE)
    tile_cols = pl.ds(col0, BWD_TILE)

    def pass_on(k, way):
        return remote(ring_ref.at[k, way], ring_ref.at[k + 1, way], ring_send.at[way, k], ring_recv.at[way, k],
                      (right, left)[way])

    def gain_copy(d):
        return remote(gains_ref.at[me], gains_ref.at[me], gain_send.at[d], gain_recv.at[d], lax.rem(me + d, n))

    def gain_arrival(d):
        src = lax.rem(me + n - d, n)
        return remote(gains_ref.at[src], gains_ref.at[src], gain_send.at[d], gain_recv.at[d], src)

    loads = [pltpu.make_async_copy(src, dst, in_sems.at[i]) for i, (src, dst) in enumerate(
        [(labels_hbm, labels_ref), (stats_hbm, stats_ref), (hidden_hbm, hidden_ref), (gain_hbm, gain_ref)])]

    @pl.when((step == 0) & (tile == 0))
    def _():
        enter(n)
        for copy in loads:
            copy.start()
        for copy in loads:
            copy.wait()

    @pl.when((step == 1) & (tile == 0))
    def _():
        entered(n)

    @pl.when((step > 0) & (tile == 0))
    def _():
        for way in range(2):
            pass_on(step - 1, way).start()

    @pl.when(tile == 0)
    def _():
        dn_ref[...] = jnp.zeros_like(dn_ref)
        labels = jnp.concatenate([labels_ref[from_r][:, 0:half], labels_ref[from_l][:, half:2 * half]], axis=1)
        label_ref[...] = row_to_col(labels) - me * vocab
        sums = jnp.concatenate([stats_ref[from_r, 0:1, 0:half], stats_ref[from_l, 0:1, half:2 * half]], axis=1)
        scale_ref[...] = row_to_col(1.0 / (sums * total))

    def logit_grads(sub):
        labels = label_ref[...] - (col0 + sub * SUB)
        iota = lax.broadcasted_iota(jnp.int32, (half, SUB), 1)
        parts = []
        for h, t_ref in enumerate((tr_ref, tl_ref)):
            rows = slice(h * half, (h + 1) * half)
            t = t_ref[:, sub * SUB:(sub + 1) * SUB]
            p = jnp.exp2(t * CAP_LOG2E) * spread(scale_ref[rows, :], SUB)
            dc = jnp.where(iota == spread(labels[rows], SUB), p - 1.0 / total, p)
            parts.append((dc * (1.0 - t * t)).astype(jnp.bfloat16))
        return jnp.concatenate(parts, axis=0)

    def add_dn(dz):
        dn_ref[...] += lax.dot_general(w_ref[...], dz, (((1,), (1,)), ((), ())), preferred_element_type=jnp.float32)

    @pl.when(tile < n_early)
    def _():
        @pl.when(step == 0)
        def _():
            dw_ref[:, tile_cols] = jnp.zeros((dw_ref.shape[0], BWD_TILE), jnp.float32)

        dz = []
        for sub in range(BWD_TILE // SUB):
            dz.append(logit_grads(sub))
            cols = pl.ds(pl.multiple_of(col0 + sub * SUB, SUB), SUB)
            dw_ref[:, cols] += jnp.dot(normed_ref[...], dz[-1], preferred_element_type=jnp.float32)
        add_dn(jnp.concatenate(dz, axis=1))

        @pl.when(step == last)
        def _():
            pltpu.make_async_copy(dw_ref.at[:, tile_cols], dw_hbm.at[:, tile_cols], dw_sems.at[tile]).start()

    @pl.when(tile >= n_early)
    def _():
        dz = jnp.concatenate([logit_grads(sub) for sub in range(BWD_TILE // SUB)], axis=1)
        dz_ref[...] = dz
        add_dn(dz)

    @pl.when((step == 0) & (tile == n_tiles - 1))
    def _():
        ring_ref[0, 0] = dn_ref[:, 0:half]
        ring_ref[0, 1] = dn_ref[:, half:2 * half]

    @pl.when((step > 0) & (tile == n_tiles - 1))
    def _():
        for way in range(2):
            pass_on(step - 1, way).wait_recv()
            ring_ref[step, way] += dn_ref[:, way * half:(way + 1) * half]

    @pl.when((step == last) & (tile == n_tiles - 1))
    def _():
        width = hidden_ref.shape[0]
        gain = 1.0 + gain_ref[...]
        folds = []
        for way in range(2):
            cols = slice(way * half, (way + 1) * half)
            x = hidden_ref[:, cols].astype(jnp.float32)
            dn = ring_ref[last, way]
            r = lax.rsqrt(jnp.mean(x * x, axis=0, keepdims=True) + EPS)
            folds.append(fold_lanes(dn * x * r))
            dy = dn * gain
            dot = jnp.sum(dy * x, axis=0, keepdims=True)
            dh_ref[:, cols] = (dy * r - x * (r * r * r * dot * (1.0 / width))).astype(dh_ref.dtype)
        gains_ref[me] = jnp.sum((folds[0] + folds[1]).T, axis=0, keepdims=True)
        dh_copy = pltpu.make_async_copy(dh_ref, dh_hbm, in_sems.at[0])
        dh_copy.start()
        for k in range(last):
            for way in range(2):
                pass_on(k, way).wait_send()
        for d in range(1, n):
            gain_copy(d).start()
        for i in range(n_early):
            cols = pl.ds(i * BWD_TILE, BWD_TILE)
            pltpu.make_async_copy(dw_ref.at[:, cols], dw_hbm.at[:, cols], dw_sems.at[i]).wait()
        dh_copy.wait()
        for d in range(1, n):
            gain_arrival(d).wait_recv()
        dgain_ref[...] = sum(gains_ref[i] for i in range(n))
        for d in range(1, n):
            gain_copy(d).wait_send()


def backward(n, labels, stats, hidden_t, gain, normed, t_r, t_l, table_t):
    _, width, chunk = normed.shape
    vocab = table_t.shape[1]
    tokens, half = n * chunk, chunk // 2
    n_tiles = vocab // BWD_TILE
    n_early = n_tiles - LATE_TILES
    early = n_early * BWD_TILE
    dma = pltpu.SemaphoreType.DMA
    return pl.pallas_call(
        functools.partial(bwd_kernel, n, n_tiles, tokens),
        grid=(n, n_tiles),
        in_specs=[
            ANY, ANY, ANY, ANY,
            pl.BlockSpec((None, width, chunk), lambda s, v: (s, 0, 0)),
            pl.BlockSpec((None, half, BWD_TILE), lambda s, v: (s, 0, v)),
            pl.BlockSpec((None, half, BWD_TILE), lambda s, v: (s, 0, v)),
            pl.BlockSpec((width, BWD_TILE), lambda s, v: (0, v)),
        ],
        out_specs=[
            ANY,
            pl.BlockSpec((None, chunk, BWD_TILE), lambda s, v: (s, 0, jnp.maximum(v - n_early, 0))),
            ANY,
            pl.BlockSpec((1, width), lambda s, v: (0, 0)),
        ],
        out_shape=[
            jax.ShapeDtypeStruct((width, early), jnp.float32),
            jax.ShapeDtypeStruct((n, chunk, vocab - early), jnp.bfloat16),
            jax.ShapeDtypeStruct((width, chunk), jnp.bfloat16),
            jax.ShapeDtypeStruct((1, width), jnp.float32),
        ],
        scratch_shapes=[
            pltpu.VMEM((width, early), jnp.float32),
            pltpu.VMEM((width, chunk), jnp.float32),
            pltpu.VMEM((n, 2, width, half), jnp.float32),
            pltpu.VMEM((chunk, LANES), jnp.int32),
            pltpu.VMEM((chunk, LANES), jnp.float32),
            pltpu.VMEM((n, 1, chunk), jnp.int32),
            pltpu.VMEM((n, 2, chunk), jnp.float32),
            pltpu.VMEM((width, chunk), jnp.bfloat16),
            pltpu.VMEM((width, 1), jnp.float32),
            pltpu.VMEM((width, chunk), jnp.bfloat16),
            pltpu.VMEM((n, 1, width), jnp.float32),
            dma((n_early,)), dma((4,)), dma((2, n)), dma((2, n)), dma((n,)), dma((n,)),
        ],
        compiler_params=pltpu.CompilerParams(vmem_limit_bytes=VMEM_LIMIT, collective_id=1, has_side_effects=True),
        cost_estimate=pl.CostEstimate(flops=4 * tokens * vocab * width, transcendentals=tokens * vocab,
                                      bytes_accessed=4 * tokens * vocab),
        name='head_bwd',
    )(labels, stats, hidden_t, gain, normed, t_r, t_l, table_t)


def late_kernel(n, early_hbm, normed_hbm, dz_hbm, dw_hbm, early_ref, normed_ref, dz_ref, dw_ref,
                early_in, early_out, normed_sems, dz_sems, out_sems):
    early, late = early_ref.shape[1], dw_ref.shape[1]
    parts = late // SUB
    piece = early // parts

    def cols_of(i, size):
        return pl.ds(pl.multiple_of(i * size, size), size)

    def fetch(i):
        return pltpu.make_async_copy(early_hbm.at[:, cols_of(i, piece)], early_ref.at[:, cols_of(i, piece)], early_in.at[i])

    def put(i):
        return pltpu.make_async_copy(early_ref.at[:, cols_of(i, piece)], dw_hbm.at[:, cols_of(i, piece)], early_out.at[i])

    def result(i):
        to = pl.ds(pl.multiple_of(early + i * SUB, SUB), SUB)
        return pltpu.make_async_copy(dw_ref.at[:, cols_of(i, SUB)], dw_hbm.at[:, to], out_sems.at[i])

    operands = [(pltpu.make_async_copy(normed_hbm.at[s], normed_ref.at[s], normed_sems.at[s]),
                 pltpu.make_async_copy(dz_hbm.at[s], dz_ref.at[s], dz_sems.at[s])) for s in range(n)]
    for pair in operands:
        for copy in pair:
            copy.start()
    for i in range(parts):
        fetch(i).start()

    def part(i, carry):
        cols = cols_of(i, SUB)
        for lo, hi in ((0, n // 4), (n // 4, n)):
            @pl.when(i == 0)
            def _(lo=lo, hi=hi):
                for pair in operands[lo:hi]:
                    for copy in pair:
                        copy.wait()

            acc = sum(jnp.dot(normed_ref[s], dz_ref[s, :, cols], preferred_element_type=jnp.float32)
                      for s in range(lo, hi))
            if lo == 0:
                dw_ref[:, cols] = acc
            else:
                dw_ref[:, cols] += acc
        result(i).start()
        fetch(i).wait()
        put(i).start()
        return carry

    lax.fori_loop(0, parts, part, 0)
    for i in range(parts):
        put(i).wait()
        result(i).wait()


def late(early_dw, normed, dz):
    n, width, chunk = normed.shape
    early, late_cols = early_dw.shape[1], dz.shape[2]
    vocab, parts = early + late_cols, late_cols // SUB
    dma = pltpu.SemaphoreType.DMA
    return pl.pallas_call(
        functools.partial(late_kernel, n),
        in_specs=[ANY, ANY, ANY],
        out_specs=ANY,
        out_shape=jax.ShapeDtypeStruct((width, vocab), jnp.float32),
        scratch_shapes=[
            pltpu.VMEM((width, early), jnp.float32),
            pltpu.VMEM((n, width, chunk), normed.dtype),
            pltpu.VMEM((n, chunk, late_cols), dz.dtype),
            pltpu.VMEM((width, late_cols), jnp.float32),
            dma((parts,)), dma((parts,)), dma((n,)), dma((n,)), dma((parts,)),
        ],
        compiler_params=pltpu.CompilerParams(vmem_limit_bytes=VMEM_LIMIT),
        cost_estimate=pl.CostEstimate(flops=2 * n * chunk * late_cols * width, transcendentals=0,
                                      bytes_accessed=8 * width * vocab),
        name='head_dw',
    )(early_dw, normed, dz)


def solution(mesh):
    n = mesh.shape[AXIS]

    def local_fn(hidden, labels, gamma, table):
        mb_dev, seq_len, width = hidden.shape
        rank = lax.axis_index(AXIS)
        own = mb_dev * seq_len
        hidden_t = hidden.reshape(own, width).T
        gain = gamma[:, None]
        table_t = table.T
        t_r, t_l, all_normed, all_labels, stats = forward(n, hidden_t, gain, labels.reshape(1, own), table_t)
        all_loss = jnp.log(stats[:, 0]) - SOFT_CAP * stats[:, 1]
        early_dw, dz, grad_hidden_t, grad_gain = backward(n, all_labels, stats, hidden_t, gain, all_normed, t_r, t_l, table_t)
        grad_table_t = late(early_dw, all_normed, dz)
        own_loss = lax.dynamic_slice_in_dim(all_loss, rank, 1, axis=0).reshape(mb_dev, seq_len)
        mean_loss = jnp.reshape(jnp.mean(all_loss), (1,))
        grad_hidden = grad_hidden_t.T.reshape(mb_dev, seq_len, width)
        return own_loss, grad_hidden, mean_loss, grad_table_t.T, grad_gain[0]

    token_spec = P(('dp', 'pp'))
    return jax.shard_map(local_fn, mesh=mesh,
                         in_specs=(token_spec, token_spec, P(), P('pp')),
                         out_specs=(token_spec, token_spec, P('dp'), token_spec, P('dp')),
                         check_vma=False)
```
